32 devices in a mesh: blk: 16 (over z, y, x), obs: 2 (over core).
Axes of the slice: x: 2, y: 2, z: 4, core: 2. Of those that a mesh axis runs over, the one named last changes fastest.
Arguments:
- populations: float32 [16, 19, 32, 1024], P('blk', None, 'obs'), may hold values from 0.011111111 to 0.533333333, as said below
- block_faces: int32 [16, 4], P('blk'), may hold values from 0 to 15, as said below
- block_edges: int32 [16, 4], P('blk'), may hold values from 0 to 15, as said below
- probe_cell: int32 [4096], P(('blk', 'obs')), may hold values from 0 to 16383
- history: bfloat16 [4096, 512], P(('blk', 'obs')), may hold values from -6 to 6
- panel_count: int32 [32], P(('blk', 'obs')), may hold values from 0 to 128, as said below
- panel_owner: int32 [4096], P(('blk', 'obs')), may hold values from 0 to 1023, as said below
- panel_pos: bfloat16 [3, 2048], P(None, ('blk', 'obs')), may hold values from -1 to 1
- panel_normal: bfloat16 [3, 2048], P(None, ('blk', 'obs')), may hold values from -0.625 to 0.625
- observers: float32 [3, 1024], P(None, 'obs'), may hold values from -8 to 8, as said below
Outputs:
- populations_out: float32 [16, 19, 32, 1024], P('blk', None, 'obs')
- spectrum: float32 [2, 512, 128], P('obs', 'blk')
The draws below stay inside these ranges and needn't reach their ends.
Inputs may be any that keep to these rules, and one draw needn't show every extreme that they name: `populations`: every population is positive. The blocks form a lattice of 4 by 4 blocks along y and z, periodic in both, one block deep in x; block_faces[b] names the blocks beside b at -y, +y, -z, +z. block_edges[b] names the blocks at (-y,-z), (-y,+z), (+y,-z), (+y,+z) of b: the y neighbour's z neighbour, which is the z neighbour's y neighbour. The eight face and edge neighbours of a block are distinct and differ from it. The live slots of a device are its first panel_count slots. The counts of the devices at one obs index sum to 1024. `panel_owner`: in a live slot of the device at blk index b and obs index o the value is q * 64 + j: slot j of the owner at blk index q and the same obs index. Every owner slot receives exactly one live panel. A device sends at most 8 live panels to one owner, and its live panels go to the owners in numbers that differ by at most one. Dead slots hold arbitrary values of the range. `observers`: every observer lies at a distance of 4 to 8 from the anchor (0, 0, 0).
All inputs are finite; a program needn't handle non-finite values.
Results may differ from the reference program's by a relative error of at most 0.0032.
The reference program's roundings to bfloat16 on the way (of `recent`, `owned`, `transform_table` and `spectra`) count: a program that leaves them out, or rounds other values in their place, can miss the bound.
Values may be sent and summed in bfloat16 or wider, within the bound.
A program may use at most 128 MiB of HBM per device.

```python
import math
import jax
import jax.numpy as jnp
from jax import lax

BS = 32
STEPS = 4
LZ = 4
SAMPLES = 256
BINS = 64
OBSERVERS = 1024
P_OWN = 64
BLOCKS = 16
LY = 4
SLAB = 16
S_DEV = 128
PANELS = 2048
SLOTS = 4096
N_OBS = 2


velocity_list = [(0, 0, 0), (1, 0, 0), (-1, 0, 0), (0, 1, 0), (0, -1, 0), (0, 0, 1), (0, 0, -1), (1, 1, 0), (-1, -1, 0), (1, -1, 0), (-1, 1, 0), (1, 0, 1), (-1, 0, -1), (1, 0, -1), (-1, 0, 1), (0, 1, 1), (0, -1, -1), (0, 1, -1), (0, -1, 1)]


weight_list = [1.0 / 3.0] + [1.0 / 18.0] * 6 + [1.0 / 36.0] * 12


def draw_populations(key, part):
    shape = (BLOCKS, 19, BS, BS * BS)
    weights = jnp.array(weight_list, jnp.float32)[None, :, None, None]
    noise = jnp.clip(jax.random.normal(key, shape, jnp.float32), -6.0, 6.0)
    return weights * (1.0 + 0.1 * noise)


def lattice(key):
    order = jax.random.permutation(jax.random.fold_in(key, 11), BLOCKS).astype(jnp.int32)
    placed = jnp.argsort(order).astype(jnp.int32)
    row_index = placed // LZ
    column_index = placed % LZ

    def beside(move_y, move_z):
        return order[(row_index + move_y) % LY * LZ + (column_index + move_z) % LZ]
    faces_list = jnp.stack([beside(-1, 0), beside(1, 0), beside(0, -1), beside(0, 1)], axis=1)
    edges_list = jnp.stack([beside(-1, -1), beside(-1, 1), beside(1, -1), beside(1, 1)], axis=1)
    return (faces_list.astype(jnp.int32), edges_list.astype(jnp.int32))


def draw_block_faces(key, part):
    return lattice(key)[0]


def draw_block_edges(key, part):
    return lattice(key)[1]


def ownership(key):
    groups = SLOTS // (S_DEV * BLOCKS)

    def one_group(subkey):
        shuffle = jax.random.permutation(jax.random.fold_in(subkey, 1), BLOCKS).astype(jnp.int32)
        halves = BLOCKS // 2
        surplus = jax.random.randint(jax.random.fold_in(subkey, 2), (halves,), 0, P_OWN + 1).astype(jnp.int32)
        surplus = surplus.at[0].set(P_OWN)
        paired = jnp.concatenate([P_OWN + surplus, P_OWN - surplus]).astype(jnp.int32)
        counts = jnp.zeros((BLOCKS,), jnp.int32).at[shuffle].set(paired)
        starts = jnp.cumsum(counts) - counts
        slot_index = jnp.arange(S_DEV, dtype=jnp.int32)
        global_rank = starts[:, None] + slot_index[None, :]
        alive_slot = slot_index[None, :] < counts[:, None]
        relabel = jax.random.permutation(jax.random.fold_in(subkey, 3), BLOCKS).astype(jnp.int32)
        spots = jax.random.permutation(jax.random.fold_in(subkey, 4), P_OWN).astype(jnp.int32)
        target = relabel[global_rank % BLOCKS]
        position = spots[jnp.minimum(global_rank // BLOCKS, P_OWN - 1)]
        filler = jax.random.randint(jax.random.fold_in(subkey, 5), (BLOCKS, S_DEV), 0, BLOCKS * P_OWN).astype(jnp.int32)
        owners = jnp.where(alive_slot, target * P_OWN + position, filler).astype(jnp.int32)
        return (counts, owners)
    counts, owners = jax.vmap(one_group)(jax.random.split(jax.random.fold_in(key, 23), groups))
    counts = counts.transpose(1, 0).reshape(-1).astype(jnp.int32)
    owners = owners.transpose(1, 0, 2).reshape(-1).astype(jnp.int32)
    return (counts, owners)


def draw_panel_count(key, part):
    return ownership(key)[0]


def draw_panel_owner(key, part):
    return ownership(key)[1]


def draw_observers(key, part):
    first_key, second_key, third_key = jax.random.split(key, 3)
    radius = jax.random.uniform(first_key, (OBSERVERS,), jnp.float32, 4.0, 8.0)
    height = jax.random.uniform(second_key, (OBSERVERS,), jnp.float32, -1.0, 1.0)
    heading = jax.random.uniform(third_key, (OBSERVERS,), jnp.float32, 0.0, 2.0 * math.pi)
    spread = jnp.sqrt(jnp.maximum(1.0 - height * height, 0.0))
    return jnp.stack([radius * spread * jnp.cos(heading), radius * spread * jnp.sin(heading), radius * height])


def with_ends(drawn, own_key, least, largest):
    spot = [jax.random.randint(jax.random.fold_in(own_key, axis), (), 0, length) for axis, length in enumerate(drawn.shape)]
    longest = drawn.shape.index(max(drawn.shape))
    neighbour = spot[:longest] + [(spot[longest] + 1) % drawn.shape[longest]] + spot[longest + 1:]
    return drawn.at[tuple(spot)].set(least).at[tuple(neighbour)].set(largest)


def block_levels(key, dims, cuts, low, largest):
    level = 1.0
    for dim, blocks in cuts:
        heights = jax.random.uniform(jax.random.fold_in(jax.random.fold_in(key, 6), dim), (blocks,), jnp.float32, low / len(cuts), largest / len(cuts))
        level = level * jnp.repeat(jnp.exp(heights), dims[dim] // blocks).reshape((-1,) + (1,) * (len(dims) - 1 - dim))
    return level


def normal_values(own_key, dims, deviation, most, pieces=(), kind=jnp.bfloat16):
    result = jax.random.normal(own_key, dims, jnp.float32) * deviation
    if len(pieces) > 0:
        result = block_levels(own_key, dims, pieces, -0.22, 0.18) * result
    return jnp.clip(result, min=-most, max=most).astype(kind)


def setup_inputs(seed: int = 0) -> dict:
    splits = jax.random.split(jax.random.key(seed), 11)
    return {
        "populations": draw_populations(jax.random.fold_in(splits[10], 71), 0),
        "block_faces": draw_block_faces(jax.random.fold_in(splits[10], 71), 0),
        "block_edges": draw_block_edges(jax.random.fold_in(splits[10], 71), 0),
        "probe_cell": with_ends(jax.random.randint(splits[3], (SLOTS,), 0, SLAB * BS * BS), jax.random.fold_in(splits[3], 1), 0, (SLAB * BS * BS) - 1).astype(jnp.int32),
        "history": normal_values(splits[4], (SLOTS, 2 * SAMPLES), 1.0, 6.0, ((0, 32),)),
        "panel_count": draw_panel_count(jax.random.fold_in(splits[10], 71), 0),
        "panel_owner": draw_panel_owner(jax.random.fold_in(splits[10], 71), 0),
        "panel_pos": jnp.clip(jax.random.uniform(splits[7], (3, PANELS), jnp.float32, -1.0, 1.0) * block_levels(splits[7], (3, PANELS), ((1, 32),), -0.4, 0.0), -1.0, 1.0).astype(jnp.bfloat16),
        "panel_normal": normal_values(splits[8], (3, PANELS), (2.0 / PANELS ** 0.5), 0.625, ((1, 32),)),
        "observers": draw_observers(jax.random.fold_in(splits[10], 71), 0),
    }


velocity_list = [(0, 0, 0), (1, 0, 0), (-1, 0, 0), (0, 1, 0), (0, -1, 0), (0, 0, 1), (0, 0, -1), (1, 1, 0), (-1, -1, 0), (1, -1, 0), (-1, 1, 0), (1, 0, 1), (-1, 0, -1), (1, 0, -1), (-1, 0, 1), (0, 1, 1), (0, -1, -1), (0, 1, -1), (0, -1, 1)]
weight_list = [1.0 / 3.0] + [1.0 / 18.0] * 6 + [1.0 / 36.0] * 12
relax_rate = 1.6
pressure_gain = 60.0
sound_speed = 0.5

def component(axis_number, extra):
    values = jnp.array([velocity[axis_number] for velocity in velocity_list], jnp.float32)
    return values.reshape((19,) + extra)

def collide(field):
    extra = (1,) * (field.ndim - 1)
    along_x = component(0, extra)
    along_y = component(1, extra)
    along_z = component(2, extra)
    weights = jnp.array(weight_list, jnp.float32).reshape((19,) + extra)
    density = lax.optimization_barrier(jnp.sum(field, axis=0))
    speed_x = lax.optimization_barrier(jnp.sum(along_x * field, axis=0)) / density
    speed_y = lax.optimization_barrier(jnp.sum(along_y * field, axis=0)) / density
    speed_z = lax.optimization_barrier(jnp.sum(along_z * field, axis=0)) / density
    projected = along_x * speed_x + along_y * speed_y + along_z * speed_z
    squared = speed_x * speed_x + speed_y * speed_y + speed_z * speed_z
    equilibrium = weights * density * (1.0 + 3.0 * projected + 4.5 * projected * projected - 1.5 * squared)
    return field + relax_rate * (equilibrium - field)

def propagate(padded):
    width_x = padded.shape[1] - 2
    width_y = padded.shape[2] - 2
    width_z = padded.shape[3] - 2
    parts = []
    for number, velocity in enumerate(velocity_list):
        shift_x, shift_y, shift_z = velocity
        parts.append(padded[number, 1 - shift_x:1 - shift_x + width_x, 1 - shift_y:1 - shift_y + width_y, 1 - shift_z:1 - shift_z + width_z])
    return jnp.stack(parts)

def pad_blocks(collided, block_faces, block_edges):
    top_index = BS - 1
    wrapped = jnp.concatenate([collided[:, :, -1:], collided, collided[:, :, :1]], axis=2)
    below_rows = wrapped[:, :, :, top_index:BS, :][block_faces[:, 0]]
    above_rows = wrapped[:, :, :, 0:1, :][block_faces[:, 1]]
    tall_block = jnp.concatenate([below_rows, wrapped, above_rows], axis=3)
    near_core = wrapped[:, :, :, :, top_index:BS][block_faces[:, 2]]
    far_core = wrapped[:, :, :, :, 0:1][block_faces[:, 3]]
    corner_ll = wrapped[:, :, :, top_index:BS, top_index:BS][block_edges[:, 0]]
    corner_lh = wrapped[:, :, :, top_index:BS, 0:1][block_edges[:, 1]]
    corner_hl = wrapped[:, :, :, 0:1, top_index:BS][block_edges[:, 2]]
    corner_hh = wrapped[:, :, :, 0:1, 0:1][block_edges[:, 3]]
    near_plane = jnp.concatenate([corner_ll, near_core, corner_hl], axis=3)
    far_plane = jnp.concatenate([corner_lh, far_core, corner_hh], axis=3)
    return jnp.concatenate([near_plane, tall_block, far_plane], axis=4)

def transform_table():
    moments = jnp.arange(SAMPLES, dtype=jnp.int32)[:, None]
    harmonics = jnp.arange(BINS, dtype=jnp.int32)[None, :] + 1
    turns = moments * harmonics % SAMPLES
    phases = turns.astype(jnp.float32) * (2.0 * math.pi / SAMPLES)
    return jnp.concatenate([jnp.cos(phases), -jnp.sin(phases)], axis=1).astype(jnp.bfloat16)

def radiate(spectra, place, normal, listen):
    values = spectra.astype(jnp.float32)
    press_real = values[0:BINS].T
    press_imag = values[BINS:2 * BINS].T
    rate_real = values[2 * BINS:3 * BINS].T
    rate_imag = values[3 * BINS:4 * BINS].T
    offsets = listen[:, None, :] - place.astype(jnp.float32)[:, :, None]
    distance_sq = lax.optimization_barrier(jnp.sum(offsets * offsets, axis=0))
    distance = jnp.sqrt(distance_sq)
    facing = lax.optimization_barrier(jnp.sum(normal.astype(jnp.float32)[:, :, None] * offsets, axis=0))
    far_term = facing / (4.0 * math.pi * sound_speed * distance_sq)
    near_term = facing / (4.0 * math.pi * distance_sq * distance)
    angular = (jnp.arange(BINS, dtype=jnp.float32) + 1.0) * (2.0 * math.pi / SAMPLES)
    phases = angular[None, :, None] * (distance / sound_speed)[:, None, :]
    cosine = jnp.cos(phases)
    sine_part = jnp.sin(phases)
    weight_real = far_term[:, None, :] * rate_real[:, :, None] + near_term[:, None, :] * press_real[:, :, None]
    weight_imag = far_term[:, None, :] * rate_imag[:, :, None] + near_term[:, None, :] * press_imag[:, :, None]
    real_part = lax.optimization_barrier(jnp.sum(weight_real * cosine + weight_imag * sine_part, axis=0))
    imag_part = lax.optimization_barrier(jnp.sum(weight_imag * cosine - weight_real * sine_part, axis=0))
    return jnp.concatenate([real_part, imag_part], axis=0).T

def reference(populations, block_faces, block_edges, probe_cell, history, panel_count, panel_owner, panel_pos, panel_normal, observers):
    field = populations.reshape(BLOCKS, 19, BS, BS, BS)
    device_of = jnp.arange(SLOTS, dtype=jnp.int32) // S_DEV
    block_of = device_of // N_OBS
    group_of = device_of % N_OBS
    depth = group_of * (BS // N_OBS) + probe_cell // (BS * BS)
    across = probe_cell % (BS * BS)
    readings = []
    for turn_index in range(STEPS):
        collided = jax.vmap(collide)(field)
        field = jax.vmap(propagate)(pad_blocks(collided, block_faces, block_edges))
        density = lax.optimization_barrier(jnp.sum(field, axis=1)).reshape(BLOCKS, BS, BS * BS)
        readings.append(density[block_of, depth, across])
    gained = pressure_gain * (jnp.stack(readings, axis=1) - 1.0)
    previous = jnp.concatenate([history[:, SAMPLES - 1:SAMPLES].astype(jnp.float32), gained[:, :-1]], axis=1)
    rate_values = gained - previous
    recent = jnp.concatenate([history[:, STEPS:SAMPLES], gained.astype(jnp.bfloat16), history[:, SAMPLES + STEPS:], rate_values.astype(jnp.bfloat16)], axis=1)
    slot_local = jnp.arange(SLOTS, dtype=jnp.int32) % S_DEV
    alive_slot = slot_local < panel_count[device_of]
    target = (panel_owner // P_OWN * N_OBS + group_of) * P_OWN + panel_owner % P_OWN
    target = jnp.where(alive_slot, target, PANELS).astype(jnp.int32)
    owned = jnp.zeros((PANELS, 2 * SAMPLES), jnp.bfloat16).at[target].set(recent, mode='drop')
    spectra = jnp.dot(owned.reshape(PANELS * 2, SAMPLES), transform_table(), preferred_element_type=jnp.float32).astype(jnp.bfloat16).reshape(PANELS, 4 * BINS)
    block_size = 256 if PANELS % 256 == 0 else PANELS
    counted = PANELS // block_size
    spectra_blocks = spectra.T.reshape(4 * BINS, counted, block_size).transpose(1, 0, 2)
    place_blocks = panel_pos.reshape(3, counted, block_size).transpose(1, 0, 2)
    normal_blocks = panel_normal.reshape(3, counted, block_size).transpose(1, 0, 2)

    def accumulate(total, inputs):
        return (total + radiate(inputs[0], inputs[1], inputs[2], observers), None)
    total, unused_out = lax.scan(accumulate, jnp.zeros((OBSERVERS, 2 * BINS), jnp.float32), (spectra_blocks, place_blocks, normal_blocks))
    return (field.reshape(BLOCKS, 19, BS, BS * BS), total.reshape(N_OBS, OBSERVERS // N_OBS, 2 * BINS))
```

```python
import math

import jax
import jax.numpy as jnp
from jax import lax
from jax.experimental import pallas as pl
from jax.experimental.pallas import tpu as pltpu
from jax.sharding import PartitionSpec as P

BS = 32
STEPS = 4
SAMPLES = 256
BINS = 64
P_OWN = 64


velocity_list = [
    (0, 0, 0),
    (1, 0, 0),
    (-1, 0, 0),
    (0, 1, 0),
    (0, -1, 0),
    (0, 0, 1),
    (0, 0, -1),
    (1, 1, 0),
    (-1, -1, 0),
    (1, -1, 0),
    (-1, 1, 0),
    (1, 0, 1),
    (-1, 0, -1),
    (1, 0, -1),
    (-1, 0, 1),
    (0, 1, 1),
    (0, -1, -1),
    (0, 1, -1),
    (0, -1, 1),
]
weight_list = [1.0 / 3.0] + [1.0 / 18.0] * 6 + [1.0 / 36.0] * 12
x_moving = [1, 2, 7, 8, 9, 10, 11, 12, 13, 14]
y_upward = [3, 7, 10, 15, 17]
y_downward = [4, 8, 9, 16, 18]
z_upward = [5, 11, 14, 15, 18]
z_downward = [6, 12, 13, 16, 17]
relax_rate = 1.6
pressure_gain = 60.0
sound_speed = 0.5


x_plus = [1, 7, 9, 11, 13]
x_minus = [2, 8, 10, 12, 14]
x_order = x_plus + x_minus
still = [0, 3, 4, 5, 6, 15, 16, 17, 18]
LANES = 128
FACE = 256


def collide_tile(f):
    density = f[0]
    for part in f[1:]:
        density = density + part
    speeds = []
    for axis in range(3):
        plus = None
        minus = None
        for number, velocity in enumerate(velocity_list):
            if velocity[axis] == 1:
                plus = f[number] if plus is None else plus + f[number]
            elif velocity[axis] == -1:
                minus = f[number] if minus is None else minus + f[number]
        speeds.append(plus - minus)
    inverse = 1.0 / density
    speeds = [speed * inverse for speed in speeds]
    squared = speeds[0] * speeds[0] + speeds[1] * speeds[1] + speeds[2] * speeds[2]
    base = 1.0 - 1.5 * squared
    scaled = {}
    for weight in sorted(set(weight_list)):
        scaled[weight] = (relax_rate * weight) * density
    out = []
    for number, velocity in enumerate(velocity_list):
        projected = None
        for axis in range(3):
            if velocity[axis] == 0:
                continue
            if projected is None:
                projected = speeds[axis] if velocity[axis] == 1 else -speeds[axis]
            elif velocity[axis] == 1:
                projected = projected + speeds[axis]
            else:
                projected = projected - speeds[axis]
        bracket = base
        if projected is not None:
            bracket = base + projected * (3.0 + 4.5 * projected)
        out.append((1.0 - relax_rate) * f[number] + scaled[weight_list[number]] * bracket)
    return out, density


def emit_collided(load, still_ref, moving_ref, up_ref, down_ref, density_ref):
    depth = still_ref.shape[1]
    for tile in range(still_ref.shape[2] // LANES):
        lanes = slice(tile * LANES, (tile + 1) * LANES)
        out, density = collide_tile([load(number, lanes) for number in range(19)])
        for place, number in enumerate(still):
            still_ref[place, :, lanes] = out[number]
        for place, number in enumerate(x_order):
            moving_ref[place, :, lanes] = out[number]
        for place, number in enumerate(x_plus):
            up_ref[place, :, lanes] = out[number][depth - 1 : depth]
        for place, number in enumerate(x_minus):
            down_ref[place, :, lanes] = out[number][0:1]
        if density_ref is not None:
            density_ref[:, lanes] = density


def first_kernel(field_ref, still_ref, moving_ref, up_ref, down_ref):
    emit_collided(
        lambda number, lanes: field_ref[number, :, lanes],
        still_ref, moving_ref, up_ref, down_ref, None,
    )


def lane_of(shape):
    return lax.broadcasted_iota(jnp.int32, shape, 1)


def turned(value, amount):
    amount = amount % value.shape[1]
    return value if amount == 0 else pltpu.roll(value, amount, 1)


def pack_kernel(target_ref, still_ref, moving_ref, low_ref, high_ref, shifted_ref, message_ref):
    depth = still_ref.shape[1]
    count = still_ref.shape[2]
    for place in range(5):
        shifted_ref[place, 0:1, :] = low_ref[place]
        shifted_ref[place, 1:depth, :] = moving_ref[place, 0 : depth - 1, :]
        shifted_ref[place + 5, depth - 1 : depth, :] = high_ref[place]
        shifted_ref[place + 5, 0 : depth - 1, :] = moving_ref[place + 5, 1:depth, :]

    def load(number, lanes):
        if number in still:
            return still_ref[still.index(number), :, lanes]
        return shifted_ref[x_order.index(number), :, lanes]

    small = lane_of((depth, LANES))
    wide = lane_of((depth, count)) % BS
    first = slice(0, LANES)
    last = slice(count - LANES, count)
    for piece, (chosen, lanes, begin) in enumerate(
        [(y_downward, first, 0), (y_upward, last, LANES - BS)]
    ):
        packed = jnp.zeros((depth, LANES), jnp.float32)
        for j in range(4):
            moved = turned(load(chosen[j], lanes), j * BS - begin)
            packed = jnp.where(small // BS == j, moved, packed)
        message_ref[target_ref[piece], :, 0:LANES] = packed
        message_ref[target_ref[piece], :, LANES:FACE] = turned(load(chosen[4], lanes), -begin)
    for piece, (chosen, begin) in enumerate([(z_downward, 0), (z_upward, BS - 1)]):
        gathered = jnp.zeros((depth, count), jnp.float32)
        for j in range(5):
            moved = turned(load(chosen[j], slice(0, count)), j - begin)
            gathered = jnp.where(wide == j, moved, gathered)
        for half in range(2):
            packed = jnp.zeros((depth, LANES), jnp.float32)
            for u in range(4):
                tile = half * 4 + u
                moved = turned(gathered[:, tile * LANES : (tile + 1) * LANES], 8 * u)
                packed = jnp.where(small % BS // 8 == u, moved, packed)
            message_ref[target_ref[2 + piece], :, half * LANES : (half + 1) * LANES] = packed
    for piece, (number, lanes) in enumerate([(16, first), (18, first), (17, last), (15, last)]):
        message_ref[target_ref[4 + piece], :, 0:LANES] = load(number, lanes)


def stream_into(target_ref, still_ref, shifted_ref, message_ref, out_ref):
    depth = still_ref.shape[1]
    count = still_ref.shape[2]
    small = lane_of((depth, LANES))
    wide = lane_of((depth, count)) % BS
    columns = []
    for piece in range(2):
        tiles = []
        for half in range(2):
            packed = message_ref[target_ref[2 + piece], :, half * LANES : (half + 1) * LANES]
            tiles += [turned(packed, -8 * u) for u in range(4)]
        columns.append(jnp.concatenate(tiles, axis=1))
    corners = {15: (4, 0, 127), 17: (5, 31, 96), 18: (6, 96, 31), 16: (7, 127, 0)}
    for number, (shift_x, shift_y, shift_z) in enumerate(velocity_list):
        if number in still:
            value = still_ref[still.index(number)]
        else:
            value = shifted_ref[x_order.index(number)]
        value = turned(value, shift_y * BS + shift_z)
        if shift_z != 0:
            chosen, piece, edge = (z_upward, 0, 0) if shift_z == 1 else (z_downward, 1, BS - 1)
            column = turned(columns[piece], edge - chosen.index(number) + BS * shift_y)
            value = jnp.where(wide == edge, column, value)
        out_ref[number] = value
        if shift_y != 0:
            chosen, piece, lanes, edge = (
                (y_upward, 0, slice(0, LANES), 0)
                if shift_y == 1
                else (y_downward, 1, slice(count - LANES, count), LANES - BS)
            )
            j = chosen.index(number)
            begin = j // 4 * LANES
            row = message_ref[target_ref[piece], :, begin : begin + LANES]
            row = turned(row, edge - j % 4 * BS + shift_z)
            keep = small // BS == edge // BS
            if shift_z != 0:
                keep = keep & (small % BS != (0 if shift_z == 1 else BS - 1))
            old = value[:, lanes]
            fixed = jnp.where(keep, row, old)
            if number in corners:
                slot, lane_to, lane_from = corners[number]
                corner = turned(message_ref[target_ref[slot], :, 0:LANES], lane_to - lane_from)
                fixed = jnp.where(small == lane_to, corner, fixed)
            out_ref[number, :, lanes] = fixed


def middle_kernel(
    target_ref, still_in, shifted_in, message_ref,
    still_ref, moving_ref, up_ref, down_ref, density_ref, field_ref,
):
    stream_into(target_ref, still_in, shifted_in, message_ref, field_ref)
    emit_collided(
        lambda number, lanes: field_ref[number, :, lanes],
        still_ref, moving_ref, up_ref, down_ref, density_ref,
    )


def last_kernel(target_ref, still_in, shifted_in, message_ref, field_ref, density_ref):
    stream_into(target_ref, still_in, shifted_in, message_ref, field_ref)
    total = field_ref[0]
    for number in range(1, 19):
        total = total + field_ref[number]
    density_ref[...] = total


def call(kernel, outs, scalars, *arrays, scratch=()):
    vmem = pl.BlockSpec(memory_space=pltpu.VMEM)
    smem = pl.BlockSpec(memory_space=pltpu.SMEM)
    shapes = [jax.ShapeDtypeStruct(shape, jnp.float32) for shape in outs]
    return pl.pallas_call(
        kernel,
        out_shape=shapes,
        in_specs=[smem] * len(scalars) + [vmem] * len(arrays),
        out_specs=[vmem] * len(outs),
        scratch_shapes=[pltpu.VMEM(shape, jnp.float32) for shape in scratch],
    )(*scalars, *arrays)


def transform_table():
    moments = jnp.arange(SAMPLES, dtype=jnp.int32)[:, None]
    harmonics = jnp.arange(BINS, dtype=jnp.int32)[None, :] + 1
    turns = moments * harmonics % SAMPLES
    phases = turns.astype(jnp.float32) * (2.0 * math.pi / SAMPLES)
    return jnp.concatenate([jnp.cos(phases), -jnp.sin(phases)], axis=1).astype(jnp.bfloat16)


def radiate_kernel(panel_ref, listen_ref, out_ref, real_ref, imag_ref):
    listeners = listen_ref.shape[1]
    real_ref[...] = jnp.zeros_like(real_ref)
    imag_ref[...] = jnp.zeros_like(imag_ref)
    step_angle = 2.0 * math.pi / SAMPLES / sound_speed

    def accumulate(block_number, carry):
        begin = pl.multiple_of(block_number * 8, 8)
        panel = panel_ref[pl.ds(begin, 8), :]
        distance_sq = None
        facing = None
        for axis in range(3):
            at = 4 * BINS + axis
            offset = listen_ref[axis : axis + 1, :] - panel[:, at : at + 1]
            square = offset * offset
            along = panel[:, at + 3 : at + 4] * offset
            distance_sq = square if distance_sq is None else distance_sq + square
            facing = along if facing is None else facing + along
        distance = jnp.sqrt(distance_sq)
        far_term = facing / (4.0 * math.pi * sound_speed * distance_sq)
        ratio = sound_speed / distance
        angle = step_angle * distance
        turn_cos = jnp.cos(angle)
        turn_sin = jnp.sin(angle)
        wave_cos = far_term * turn_cos
        wave_sin = far_term * turn_sin
        for k in range(BINS):
            press_real = panel[:, k : k + 1]
            press_imag = panel[:, BINS + k : BINS + k + 1]
            rate_real = panel[:, 2 * BINS + k : 2 * BINS + k + 1]
            rate_imag = panel[:, 3 * BINS + k : 3 * BINS + k + 1]
            mixed_real = rate_real + ratio * press_real
            mixed_imag = rate_imag + ratio * press_imag
            real_ref[k] += mixed_real * wave_cos + mixed_imag * wave_sin
            imag_ref[k] += mixed_imag * wave_cos - mixed_real * wave_sin
            if k + 1 < BINS:
                wave_cos, wave_sin = (
                    wave_cos * turn_cos - wave_sin * turn_sin,
                    wave_sin * turn_cos + wave_cos * turn_sin,
                )
        return carry

    lax.fori_loop(0, panel_ref.shape[0] // 8, accumulate, 0)
    both = jnp.concatenate([jnp.sum(real_ref[...], axis=1), jnp.sum(imag_ref[...], axis=1)], axis=0)
    out_ref[...] = both.T


def route_slots(payload, owners, alive_slot, blocks):
    count_slots = payload.shape[0]
    capacity = -(-count_slots // blocks)
    target = owners // P_OWN
    member = (
        (target[:, None] == jnp.arange(blocks, dtype=jnp.int32)[None, :]) & alive_slot[:, None]
    ).astype(jnp.int32)
    before = jnp.cumsum(member, axis=0) - member
    order_within = jnp.sum(before * member, axis=1)
    slot_label = jnp.where(alive_slot, target * capacity + order_within, -1)
    matches = slot_label[:, None] == jnp.arange(blocks * capacity, dtype=jnp.int32)[None, :]
    source = jnp.sum(
        jnp.where(matches, jnp.arange(count_slots, dtype=jnp.int32)[:, None], 0), axis=0
    )
    filled = jnp.any(matches, axis=0)
    outgoing = jnp.take(payload, source, axis=0).reshape(blocks, capacity, payload.shape[1])
    spots = jnp.where(filled, jnp.take(owners, source) % P_OWN, -1).reshape(blocks, capacity, 1)
    return jnp.concatenate([outgoing, spots.astype(jnp.bfloat16)], axis=2)


def settle(incoming):
    width = incoming.shape[-1] - 1
    flat = incoming.reshape(-1, width + 1)
    spots = flat[:, width].astype(jnp.int32)
    choose = (spots[:, None] == jnp.arange(P_OWN, dtype=jnp.int32)[None, :]).astype(jnp.bfloat16)
    return jnp.einsum(
        "rp,rw->pw", choose, flat[:, :width], preferred_element_type=jnp.float32
    ).astype(jnp.bfloat16)


def body(
    populations,
    block_faces,
    block_edges,
    probe_cell,
    history,
    panel_count,
    panel_owner,
    panel_pos,
    panel_normal,
    observers,
):
    blocks = lax.axis_size("blk")
    lattice_state = populations[0]
    slab_depth = lattice_state.shape[1]
    lane_count = lattice_state.shape[2]
    targets = jnp.concatenate([block_faces[0], block_edges[0]])
    ring = lax.axis_size("obs")
    forward = [(i, (i + 1) % ring) for i in range(ring)]
    backward = [(target, source) for source, target in forward]
    still_shape = (len(still), slab_depth, lane_count)
    moving_shape = (len(x_order), slab_depth, lane_count)
    edge_shape = (5, 1, lane_count)
    collided_shapes = [still_shape, moving_shape, edge_shape, edge_shape]
    plane_shape = (slab_depth, lane_count)
    field_shape = (19, slab_depth, lane_count)
    still_part, moving_part, up, down = call(first_kernel, collided_shapes, (), lattice_state)
    densities = []
    for turn_index in range(STEPS):
        low = lax.ppermute(up, "obs", forward)
        high = lax.ppermute(down, "obs", backward)
        shifted, outgoing = call(
            pack_kernel,
            [moving_shape, (blocks, slab_depth, FACE)],
            (targets,), still_part, moving_part, low, high,
        )
        received = lax.all_to_all(outgoing, "blk", split_axis=0, concat_axis=0, tiled=True)
        if turn_index + 1 < STEPS:
            still_part, moving_part, up, down, density = call(
                middle_kernel,
                collided_shapes + [plane_shape],
                (targets,), still_part, shifted, received,
                scratch=[field_shape],
            )
        else:
            lattice_state, density = call(
                last_kernel, [field_shape, plane_shape], (targets,), still_part, shifted, received
            )
        densities.append(density)
    populations_out = lattice_state.reshape(1, 19, slab_depth, lane_count)
    readings = [jnp.take(density.reshape(-1), probe_cell) for density in densities]
    gained = pressure_gain * (jnp.stack(readings, axis=1) - 1.0)
    previous = jnp.concatenate(
        [history[:, SAMPLES - 1 : SAMPLES].astype(jnp.float32), gained[:, :-1]], axis=1
    )
    rate_values = gained - previous
    recent = jnp.concatenate(
        [
            history[:, STEPS:SAMPLES],
            gained.astype(jnp.bfloat16),
            history[:, SAMPLES + STEPS :],
            rate_values.astype(jnp.bfloat16),
        ],
        axis=1,
    )
    transform = transform_table()
    count_slots = recent.shape[0]
    alive_slot = jnp.arange(count_slots, dtype=jnp.int32) < panel_count[0]
    outgoing = route_slots(recent, panel_owner, alive_slot, blocks)
    incoming = lax.all_to_all(outgoing, "blk", split_axis=0, concat_axis=0, tiled=True)
    owned = settle(incoming).reshape(P_OWN, 2, SAMPLES)
    spectra = (
        jnp.einsum("pgt,tk->pgk", owned, transform, preferred_element_type=jnp.float32)
        .astype(jnp.bfloat16)
        .reshape(P_OWN, 4 * BINS)
    )
    panels = jnp.concatenate([spectra, panel_pos.T, panel_normal.T], axis=1)
    gathered = lax.all_gather(panels, "obs", axis=0, tiled=True).astype(jnp.float32)
    listeners = observers.shape[1]
    partial_value = call(
        radiate_kernel,
        [(listeners, 2 * BINS)],
        (), gathered, observers,
        scratch=[(BINS, 8, listeners), (BINS, 8, listeners)],
    )[0]
    pieces = lax.all_to_all(
        partial_value.reshape(blocks, listeners // blocks, 2 * BINS),
        "blk", split_axis=0, concat_axis=0, tiled=True,
    )
    return (populations_out, jnp.sum(pieces, axis=0)[None])


def solution(mesh):
    placed = (
        P("blk", None, "obs", None),
        P("blk", None),
        P("blk", None),
        P(("blk", "obs")),
        P(("blk", "obs"), None),
        P(("blk", "obs")),
        P(("blk", "obs")),
        P(None, ("blk", "obs")),
        P(None, ("blk", "obs")),
        P(None, "obs"),
    )
    return jax.shard_map(
        body,
        mesh=mesh,
        in_specs=placed,
        out_specs=(P("blk", None, "obs", None), P("obs", "blk", None)),
        check_vma=False,
    )
```

```python
import functools
import math

import jax
import jax.numpy as jnp
from jax import lax
from jax.experimental import pallas as pl
from jax.experimental.pallas import tpu as pltpu
from jax.sharding import PartitionSpec as P

BS = 32
STEPS = 4
SAMPLES = 256
BINS = 64
P_OWN = 64


velocity_list = [
    (0, 0, 0),
    (1, 0, 0),
    (-1, 0, 0),
    (0, 1, 0),
    (0, -1, 0),
    (0, 0, 1),
    (0, 0, -1),
    (1, 1, 0),
    (-1, -1, 0),
    (1, -1, 0),
    (-1, 1, 0),
    (1, 0, 1),
    (-1, 0, -1),
    (1, 0, -1),
    (-1, 0, 1),
    (0, 1, 1),
    (0, -1, -1),
    (0, 1, -1),
    (0, -1, 1),
]
weight_list = [1.0 / 3.0] + [1.0 / 18.0] * 6 + [1.0 / 36.0] * 12
x_moving = [1, 2, 7, 8, 9, 10, 11, 12, 13, 14]
y_upward = [3, 7, 10, 15, 17]
y_downward = [4, 8, 9, 16, 18]
z_upward = [5, 11, 14, 15, 18]
z_downward = [6, 12, 13, 16, 17]
relax_rate = 1.6
pressure_gain = 60.0
sound_speed = 0.5


x_plus = [1, 7, 9, 11, 13]
x_minus = [2, 8, 10, 12, 14]
x_order = x_plus + x_minus
still = [0, 3, 4, 5, 6, 15, 16, 17, 18]
LANES = 128
FACE = 256


def collide_tile(f):
    density = f[0]
    for part in f[1:]:
        density = density + part
    speeds = []
    for axis in range(3):
        plus = None
        minus = None
        for number, velocity in enumerate(velocity_list):
            if velocity[axis] == 1:
                plus = f[number] if plus is None else plus + f[number]
            elif velocity[axis] == -1:
                minus = f[number] if minus is None else minus + f[number]
        speeds.append(plus - minus)
    inverse = 1.0 / density
    speeds = [speed * inverse for speed in speeds]
    squared = speeds[0] * speeds[0] + speeds[1] * speeds[1] + speeds[2] * speeds[2]
    base = 1.0 - 1.5 * squared
    scaled = {}
    for weight in sorted(set(weight_list)):
        scaled[weight] = (relax_rate * weight) * density
    out = []
    for number, velocity in enumerate(velocity_list):
        projected = None
        for axis in range(3):
            if velocity[axis] == 0:
                continue
            if projected is None:
                projected = speeds[axis] if velocity[axis] == 1 else -speeds[axis]
            elif velocity[axis] == 1:
                projected = projected + speeds[axis]
            else:
                projected = projected - speeds[axis]
        bracket = base
        if projected is not None:
            bracket = base + projected * (3.0 + 4.5 * projected)
        out.append((1.0 - relax_rate) * f[number] + scaled[weight_list[number]] * bracket)
    return out, density


def collide_all(field_ref, still_ref, moving_ref, up_ref, down_ref):
    depth = still_ref.shape[1]

    def one_tile(tile, carry):
        lanes = pl.ds(pl.multiple_of(tile * LANES, LANES), LANES)
        out = collide_tile([field_ref[number, :, lanes] for number in range(19)])[0]
        for place, number in enumerate(still):
            still_ref[place, :, lanes] = out[number]
        for place, number in enumerate(x_order):
            moving_ref[place, :, lanes] = out[number]
        for place, number in enumerate(x_plus):
            up_ref[place, :, lanes] = out[number][depth - 1 : depth]
        for place, number in enumerate(x_minus):
            down_ref[place, :, lanes] = out[number][0:1]
        return carry

    lax.fori_loop(0, still_ref.shape[2] // LANES, one_tile, 0)


def lane_of(shape):
    return lax.broadcasted_iota(jnp.int32, shape, 1)


def turned(value, amount):
    amount = amount % value.shape[1]
    return value if amount == 0 else pltpu.roll(value, amount, 1)


def pack_pieces(still_ref, moving_ref, low_ref, high_ref, shifted_ref, piece_ref):
    depth = still_ref.shape[1]
    count = still_ref.shape[2]
    for place in range(5):
        shifted_ref[place, 0:1, :] = low_ref[place]
        shifted_ref[place, 1:depth, :] = moving_ref[place, 0 : depth - 1, :]
        shifted_ref[place + 5, depth - 1 : depth, :] = high_ref[place]
        shifted_ref[place + 5, 0 : depth - 1, :] = moving_ref[place + 5, 1:depth, :]

    def load(number, lanes):
        if number in still:
            return still_ref[still.index(number), :, lanes]
        return shifted_ref[x_order.index(number), :, lanes]

    small = lane_of((depth, LANES))
    wide = lane_of((depth, count)) % BS
    first = slice(0, LANES)
    last = slice(count - LANES, count)
    for piece, (chosen, lanes, begin) in enumerate(
        [(y_downward, first, 0), (y_upward, last, LANES - BS)]
    ):
        packed = jnp.zeros((depth, LANES), jnp.float32)
        for j in range(4):
            moved = turned(load(chosen[j], lanes), j * BS - begin)
            packed = jnp.where(small // BS == j, moved, packed)
        piece_ref[piece, :, 0:LANES] = packed
        piece_ref[piece, :, LANES:FACE] = turned(load(chosen[4], lanes), -begin)
    for piece, (chosen, begin) in enumerate([(z_downward, 0), (z_upward, BS - 1)]):
        gathered = jnp.zeros((depth, count), jnp.float32)
        for j in range(5):
            moved = turned(load(chosen[j], slice(0, count)), j - begin)
            gathered = jnp.where(wide == j, moved, gathered)
        for half in range(2):
            packed = jnp.zeros((depth, LANES), jnp.float32)
            for u in range(4):
                tile = half * 4 + u
                moved = turned(gathered[:, tile * LANES : (tile + 1) * LANES], 8 * u)
                packed = jnp.where(small % BS // 8 == u, moved, packed)
            piece_ref[2 + piece, :, half * LANES : (half + 1) * LANES] = packed
    for piece, (number, lanes) in enumerate([(16, first), (18, first), (17, last), (15, last)]):
        piece_ref[4 + piece, :, 0:LANES] = load(number, lanes)


def stream_into(still_ref, shifted_ref, message_ref, out_ref):
    depth = still_ref.shape[1]
    count = still_ref.shape[2]
    small = lane_of((depth, LANES))
    wide = lane_of((depth, count)) % BS
    columns = []
    for piece in range(2):
        tiles = []
        for half in range(2):
            packed = message_ref[2 + piece, :, half * LANES : (half + 1) * LANES]
            tiles += [turned(packed, -8 * u) for u in range(4)]
        columns.append(jnp.concatenate(tiles, axis=1))
    corners = {15: (4, 0, 127), 17: (5, 31, 96), 18: (6, 96, 31), 16: (7, 127, 0)}
    for number, (shift_x, shift_y, shift_z) in enumerate(velocity_list):
        if number in still:
            value = still_ref[still.index(number)]
        else:
            value = shifted_ref[x_order.index(number)]
        value = turned(value, shift_y * BS + shift_z)
        if shift_z != 0:
            chosen, piece, edge = (z_upward, 0, 0) if shift_z == 1 else (z_downward, 1, BS - 1)
            column = turned(columns[piece], edge - chosen.index(number) + BS * shift_y)
            value = jnp.where(wide == edge, column, value)
        out_ref[number] = value
        if shift_y != 0:
            chosen, piece, lanes, edge = (
                (y_upward, 0, slice(0, LANES), 0)
                if shift_y == 1
                else (y_downward, 1, slice(count - LANES, count), LANES - BS)
            )
            j = chosen.index(number)
            begin = j // 4 * LANES
            row = message_ref[piece, :, begin : begin + LANES]
            row = turned(row, edge - j % 4 * BS + shift_z)
            keep = small // BS == edge // BS
            if shift_z != 0:
                keep = keep & (small % BS != (0 if shift_z == 1 else BS - 1))
            old = value[:, lanes]
            fixed = jnp.where(keep, row, old)
            if number in corners:
                slot, lane_to, lane_from = corners[number]
                corner = turned(message_ref[slot, :, 0:LANES], lane_to - lane_from)
                fixed = jnp.where(small == lane_to, corner, fixed)
            out_ref[number, :, lanes] = fixed


def window_kernel(
    blocks, ring, target_ref, start_ref, field_ref, density_ref,
    still_ref, moving_ref, shifted_ref, up_ref, down_ref, low_ref, high_ref,
    piece_ref, send_ref, got_ref, edge_send, edge_got, send_sem, got_sem,
):
    mesh_ids = pl.DeviceIdType.MESH
    me = lax.axis_index("blk")
    side = lax.axis_index("obs")
    right = lax.rem(side + 1, ring)
    left = lax.rem(side + ring - 1, ring)
    barrier = pltpu.get_barrier_semaphore()

    def greet(distance, carry):
        peer = lax.rem(me + distance, blocks)
        pl.semaphore_signal(barrier, inc=1, device_id=(peer, side), device_id_type=mesh_ids)
        return carry

    for beside in (left, right):
        pl.semaphore_signal(barrier, inc=1, device_id=(me, beside), device_id_type=mesh_ids)
    lax.fori_loop(1, blocks, greet, 0)
    field_ref[...] = start_ref[...]
    pl.semaphore_wait(barrier, blocks + 1)

    def one_step(step, carry):
        collide_all(field_ref, still_ref, moving_ref, up_ref, down_ref)
        edges = [
            pltpu.make_async_remote_copy(
                src_ref=source,
                dst_ref=into.at[step],
                send_sem=edge_send.at[step, way],
                recv_sem=edge_got.at[step, way],
                device_id=(me, beside),
                device_id_type=mesh_ids,
            )
            for way, (source, into, beside) in enumerate(
                [(up_ref, low_ref, right), (down_ref, high_ref, left)]
            )
        ]
        for edge in edges:
            edge.start()
        for edge in edges:
            edge.wait()
        pack_pieces(
            still_ref, moving_ref, low_ref.at[step], high_ref.at[step], shifted_ref, piece_ref
        )

        def copy_to(distance):
            return pltpu.make_async_remote_copy(
                src_ref=send_ref.at[distance],
                dst_ref=got_ref.at[step, me],
                send_sem=send_sem.at[step, distance],
                recv_sem=got_sem.at[step, distance],
                device_id=(lax.rem(me + distance, blocks), side),
                device_id_type=mesh_ids,
            )

        def fill(distance, inner):
            peer = lax.rem(me + distance, blocks)
            near = jnp.zeros((send_ref.shape[1], LANES), jnp.float32)
            rest = near
            for piece in range(8):
                wanted = target_ref[piece] == peer
                near = jnp.where(wanted, piece_ref[piece, :, 0:LANES], near)
                if piece < 4:
                    rest = jnp.where(wanted, piece_ref[piece, :, LANES:FACE], rest)
            send_ref[distance, :, 0:LANES] = near
            send_ref[distance, :, LANES:FACE] = rest
            return inner

        def begin(distance, inner):
            copy_to(distance).start()
            return inner

        def finish(distance, inner):
            copy_to(distance).wait()
            return inner

        lax.fori_loop(1, blocks, fill, 0)
        lax.fori_loop(1, blocks, begin, 0)
        lax.fori_loop(1, blocks, finish, 0)

        def choose(distance, held):
            peer = lax.rem(me + distance, blocks)
            near = got_ref[step, peer, :, 0:LANES]
            rest = got_ref[step, peer, :, LANES:FACE]
            wanted = [target_ref[piece] == peer for piece in range(8)]
            return tuple(
                jnp.where(wanted[at % 8], near if at < 8 else rest, held[at]) for at in range(12)
            )

        blank = jnp.zeros((send_ref.shape[1], LANES), jnp.float32)
        held = lax.fori_loop(1, blocks, choose, (blank,) * 12)
        for at in range(12):
            half = at // 8 * LANES
            piece_ref[at % 8, :, half : half + LANES] = held[at]
        stream_into(still_ref, shifted_ref, piece_ref, field_ref)
        total = field_ref[0]
        for number in range(1, 19):
            total = total + field_ref[number]
        density_ref[step] = total
        return carry

    lax.fori_loop(0, STEPS, one_step, 0)


def call(kernel, outs, scalars, *arrays, scratch=()):
    vmem = pl.BlockSpec(memory_space=pltpu.VMEM)
    smem = pl.BlockSpec(memory_space=pltpu.SMEM)
    shapes = [jax.ShapeDtypeStruct(shape, jnp.float32) for shape in outs]
    return pl.pallas_call(
        kernel,
        out_shape=shapes,
        in_specs=[smem] * len(scalars) + [vmem] * len(arrays),
        out_specs=[vmem] * len(outs),
        scratch_shapes=[pltpu.VMEM(shape, jnp.float32) for shape in scratch],
    )(*scalars, *arrays)


def transform_table():
    moments = jnp.arange(SAMPLES, dtype=jnp.int32)[:, None]
    harmonics = jnp.arange(BINS, dtype=jnp.int32)[None, :] + 1
    turns = moments * harmonics % SAMPLES
    phases = turns.astype(jnp.float32) * (2.0 * math.pi / SAMPLES)
    return jnp.concatenate([jnp.cos(phases), -jnp.sin(phases)], axis=1).astype(jnp.bfloat16)


def radiate_kernel(panel_ref, listen_ref, out_ref, real_ref, imag_ref):
    listeners = listen_ref.shape[1]
    real_ref[...] = jnp.zeros_like(real_ref)
    imag_ref[...] = jnp.zeros_like(imag_ref)
    step_angle = 2.0 * math.pi / SAMPLES / sound_speed

    def accumulate(block_number, carry):
        begin = pl.multiple_of(block_number * 8, 8)
        panel = panel_ref[pl.ds(begin, 8), :]
        distance_sq = None
        facing = None
        for axis in range(3):
            at = 4 * BINS + axis
            offset = listen_ref[axis : axis + 1, :] - panel[:, at : at + 1]
            square = offset * offset
            along = panel[:, at + 3 : at + 4] * offset
            distance_sq = square if distance_sq is None else distance_sq + square
            facing = along if facing is None else facing + along
        distance = jnp.sqrt(distance_sq)
        far_term = facing / (4.0 * math.pi * sound_speed * distance_sq)
        ratio = sound_speed / distance
        angle = step_angle * distance
        turn_cos = jnp.cos(angle)
        turn_sin = jnp.sin(angle)
        wave_cos = far_term * turn_cos
        wave_sin = far_term * turn_sin
        for k in range(BINS):
            press_real = panel[:, k : k + 1]
            press_imag = panel[:, BINS + k : BINS + k + 1]
            rate_real = panel[:, 2 * BINS + k : 2 * BINS + k + 1]
            rate_imag = panel[:, 3 * BINS + k : 3 * BINS + k + 1]
            mixed_real = rate_real + ratio * press_real
            mixed_imag = rate_imag + ratio * press_imag
            real_ref[k] += mixed_real * wave_cos + mixed_imag * wave_sin
            imag_ref[k] += mixed_imag * wave_cos - mixed_real * wave_sin
            if k + 1 < BINS:
                wave_cos, wave_sin = (
                    wave_cos * turn_cos - wave_sin * turn_sin,
                    wave_sin * turn_cos + wave_cos * turn_sin,
                )
        return carry

    lax.fori_loop(0, panel_ref.shape[0] // 8, accumulate, 0)
    both = jnp.concatenate([jnp.sum(real_ref[...], axis=1), jnp.sum(imag_ref[...], axis=1)], axis=0)
    out_ref[...] = both.T


def route_slots(payload, owners, alive_slot, blocks):
    count_slots = payload.shape[0]
    capacity = -(-count_slots // blocks)
    target = owners // P_OWN
    member = (
        (target[:, None] == jnp.arange(blocks, dtype=jnp.int32)[None, :]) & alive_slot[:, None]
    ).astype(jnp.int32)
    before = jnp.cumsum(member, axis=0) - member
    order_within = jnp.sum(before * member, axis=1)
    slot_label = jnp.where(alive_slot, target * capacity + order_within, -1)
    matches = slot_label[:, None] == jnp.arange(blocks * capacity, dtype=jnp.int32)[None, :]
    source = jnp.sum(
        jnp.where(matches, jnp.arange(count_slots, dtype=jnp.int32)[:, None], 0), axis=0
    )
    filled = jnp.any(matches, axis=0)
    outgoing = jnp.take(payload, source, axis=0).reshape(blocks, capacity, payload.shape[1])
    spots = jnp.where(filled, jnp.take(owners, source) % P_OWN, -1).reshape(blocks, capacity, 1)
    return jnp.concatenate([outgoing, spots.astype(jnp.bfloat16)], axis=2)


def settle(incoming):
    width = incoming.shape[-1] - 1
    flat = incoming.reshape(-1, width + 1)
    spots = flat[:, width].astype(jnp.int32)
    choose = (spots[:, None] == jnp.arange(P_OWN, dtype=jnp.int32)[None, :]).astype(jnp.bfloat16)
    return jnp.einsum(
        "rp,rw->pw", choose, flat[:, :width], preferred_element_type=jnp.float32
    ).astype(jnp.bfloat16)


def body(
    populations,
    block_faces,
    block_edges,
    probe_cell,
    history,
    panel_count,
    panel_owner,
    panel_pos,
    panel_normal,
    observers,
):
    blocks = lax.axis_size("blk")
    lattice_state = populations[0]
    slab_depth = lattice_state.shape[1]
    lane_count = lattice_state.shape[2]
    targets = jnp.concatenate([block_faces[0], block_edges[0]])
    ring = lax.axis_size("obs")
    still_shape = (len(still), slab_depth, lane_count)
    moving_shape = (len(x_order), slab_depth, lane_count)
    edge_shape = (5, 1, lane_count)
    vmem = pl.BlockSpec(memory_space=pltpu.VMEM)
    scratch = [
        still_shape, moving_shape, moving_shape, edge_shape, edge_shape,
        (STEPS,) + edge_shape, (STEPS,) + edge_shape,
        (8, slab_depth, FACE), (blocks, slab_depth, FACE), (STEPS, blocks, slab_depth, FACE),
    ]
    lattice_state, densities = pl.pallas_call(
        functools.partial(window_kernel, blocks, ring),
        out_shape=[
            jax.ShapeDtypeStruct((19, slab_depth, lane_count), jnp.float32),
            jax.ShapeDtypeStruct((STEPS, slab_depth, lane_count), jnp.float32),
        ],
        in_specs=[pl.BlockSpec(memory_space=pltpu.SMEM), vmem],
        out_specs=[vmem, vmem],
        scratch_shapes=[pltpu.VMEM(shape, jnp.float32) for shape in scratch]
        + [pltpu.SemaphoreType.DMA((STEPS, 2))] * 2
        + [pltpu.SemaphoreType.DMA((STEPS, blocks))] * 2,
        compiler_params=pltpu.CompilerParams(collective_id=0, has_side_effects=True),
    )(targets, lattice_state)
    populations_out = lattice_state.reshape(1, 19, slab_depth, lane_count)
    readings = [jnp.take(density.reshape(-1), probe_cell) for density in densities]
    gained = pressure_gain * (jnp.stack(readings, axis=1) - 1.0)
    previous = jnp.concatenate(
        [history[:, SAMPLES - 1 : SAMPLES].astype(jnp.float32), gained[:, :-1]], axis=1
    )
    rate_values = gained - previous
    recent = jnp.concatenate(
        [
            history[:, STEPS:SAMPLES],
            gained.astype(jnp.bfloat16),
            history[:, SAMPLES + STEPS :],
            rate_values.astype(jnp.bfloat16),
        ],
        axis=1,
    )
    transform = transform_table()
    count_slots = recent.shape[0]
    alive_slot = jnp.arange(count_slots, dtype=jnp.int32) < panel_count[0]
    outgoing = route_slots(recent, panel_owner, alive_slot, blocks)
    incoming = lax.all_to_all(outgoing, "blk", split_axis=0, concat_axis=0, tiled=True)
    owned = settle(incoming).reshape(P_OWN, 2, SAMPLES)
    spectra = (
        jnp.einsum("pgt,tk->pgk", owned, transform, preferred_element_type=jnp.float32)
        .astype(jnp.bfloat16)
        .reshape(P_OWN, 4 * BINS)
    )
    panels = jnp.concatenate([spectra, panel_pos.T, panel_normal.T], axis=1)
    gathered = lax.all_gather(panels, "obs", axis=0, tiled=True).astype(jnp.float32)
    listeners = observers.shape[1]
    partial_value = call(
        radiate_kernel,
        [(listeners, 2 * BINS)],
        (), gathered, observers,
        scratch=[(BINS, 8, listeners), (BINS, 8, listeners)],
    )[0]
    pieces = lax.all_to_all(
        partial_value.reshape(blocks, listeners // blocks, 2 * BINS),
        "blk", split_axis=0, concat_axis=0, tiled=True,
    )
    return (populations_out, jnp.sum(pieces, axis=0)[None])


def solution(mesh):
    placed = (
        P("blk", None, "obs", None),
        P("blk", None),
        P("blk", None),
        P(("blk", "obs")),
        P(("blk", "obs"), None),
        P(("blk", "obs")),
        P(("blk", "obs")),
        P(None, ("blk", "obs")),
        P(None, ("blk", "obs")),
        P(None, "obs"),
    )
    return jax.shard_map(
        body,
        mesh=mesh,
        in_specs=placed,
        out_specs=(P("blk", None, "obs", None), P("obs", "blk", None)),
        check_vma=False,
    )
```

```python
import functools
import math

import jax
import jax.numpy as jnp
from jax import lax
from jax.experimental import pallas as pl
from jax.experimental.pallas import tpu as pltpu
from jax.sharding import PartitionSpec as P

BS = 32
STEPS = 4
SAMPLES = 256
BINS = 64
P_OWN = 64


velocity_list = [
    (0, 0, 0),
    (1, 0, 0),
    (-1, 0, 0),
    (0, 1, 0),
    (0, -1, 0),
    (0, 0, 1),
    (0, 0, -1),
    (1, 1, 0),
    (-1, -1, 0),
    (1, -1, 0),
    (-1, 1, 0),
    (1, 0, 1),
    (-1, 0, -1),
    (1, 0, -1),
    (-1, 0, 1),
    (0, 1, 1),
    (0, -1, -1),
    (0, 1, -1),
    (0, -1, 1),
]
weight_list = [1.0 / 3.0] + [1.0 / 18.0] * 6 + [1.0 / 36.0] * 12
x_moving = [1, 2, 7, 8, 9, 10, 11, 12, 13, 14]
y_upward = [3, 7, 10, 15, 17]
y_downward = [4, 8, 9, 16, 18]
z_upward = [5, 11, 14, 15, 18]
z_downward = [6, 12, 13, 16, 17]
relax_rate = 1.6
pressure_gain = 60.0
sound_speed = 0.5


x_plus = [1, 7, 9, 11, 13]
x_minus = [2, 8, 10, 12, 14]
x_order = x_plus + x_minus
still = [0, 3, 4, 5, 6, 15, 16, 17, 18]
LANES = 128
FACE = 256


def collide_tile(f):
    density = f[0]
    for part in f[1:]:
        density = density + part
    speeds = []
    for axis in range(3):
        plus = None
        minus = None
        for number, velocity in enumerate(velocity_list):
            if velocity[axis] == 1:
                plus = f[number] if plus is None else plus + f[number]
            elif velocity[axis] == -1:
                minus = f[number] if minus is None else minus + f[number]
        speeds.append(plus - minus)
    inverse = 1.0 / density
    speeds = [speed * inverse for speed in speeds]
    squared = speeds[0] * speeds[0] + speeds[1] * speeds[1] + speeds[2] * speeds[2]
    base = 1.0 - 1.5 * squared
    scaled = {}
    for weight in sorted(set(weight_list)):
        scaled[weight] = (relax_rate * weight) * density
    out = []
    for number, velocity in enumerate(velocity_list):
        projected = None
        for axis in range(3):
            if velocity[axis] == 0:
                continue
            if projected is None:
                projected = speeds[axis] if velocity[axis] == 1 else -speeds[axis]
            elif velocity[axis] == 1:
                projected = projected + speeds[axis]
            else:
                projected = projected - speeds[axis]
        bracket = base
        if projected is not None:
            bracket = base + projected * (3.0 + 4.5 * projected)
        out.append((1.0 - relax_rate) * f[number] + scaled[weight_list[number]] * bracket)
    return out, density


def collide_all(field_ref, still_ref, moving_ref, up_ref, down_ref):
    depth = still_ref.shape[1]

    def one_tile(tile, carry):
        lanes = pl.ds(pl.multiple_of(tile * LANES, LANES), LANES)
        out = collide_tile([field_ref[number, :, lanes] for number in range(19)])[0]
        for place, number in enumerate(still):
            still_ref[place, :, lanes] = out[number]
        for place, number in enumerate(x_order):
            moving_ref[place, :, lanes] = out[number]
        for place, number in enumerate(x_plus):
            up_ref[place, :, lanes] = out[number][depth - 1 : depth]
        for place, number in enumerate(x_minus):
            down_ref[place, :, lanes] = out[number][0:1]
        return carry

    lax.fori_loop(0, still_ref.shape[2] // LANES, one_tile, 0)


def lane_of(shape):
    return lax.broadcasted_iota(jnp.int32, shape, 1)


def turned(value, amount):
    amount = amount % value.shape[1]
    return value if amount == 0 else pltpu.roll(value, amount, 1)


def pack_pieces(still_ref, moving_ref, low_ref, high_ref, shifted_ref, piece_ref):
    depth = still_ref.shape[1]
    count = still_ref.shape[2]
    for place in range(5):
        shifted_ref[place, 0:1, :] = low_ref[place]
        shifted_ref[place, 1:depth, :] = moving_ref[place, 0 : depth - 1, :]
        shifted_ref[place + 5, depth - 1 : depth, :] = high_ref[place]
        shifted_ref[place + 5, 0 : depth - 1, :] = moving_ref[place + 5, 1:depth, :]

    def load(number, lanes):
        if number in still:
            return still_ref[still.index(number), :, lanes]
        return shifted_ref[x_order.index(number), :, lanes]

    small = lane_of((depth, LANES))
    wide = lane_of((depth, count)) % BS
    first = slice(0, LANES)
    last = slice(count - LANES, count)
    for piece, (chosen, lanes, begin) in enumerate(
        [(y_downward, first, 0), (y_upward, last, LANES - BS)]
    ):
        packed = jnp.zeros((depth, LANES), jnp.float32)
        for j in range(4):
            moved = turned(load(chosen[j], lanes), j * BS - begin)
            packed = jnp.where(small // BS == j, moved, packed)
        piece_ref[piece, :, 0:LANES] = packed
        piece_ref[piece, :, LANES:FACE] = turned(load(chosen[4], lanes), -begin)
    for piece, (chosen, begin) in enumerate([(z_downward, 0), (z_upward, BS - 1)]):
        gathered = jnp.zeros((depth, count), jnp.float32)
        for j in range(5):
            moved = turned(load(chosen[j], slice(0, count)), j - begin)
            gathered = jnp.where(wide == j, moved, gathered)
        for half in range(2):
            packed = jnp.zeros((depth, LANES), jnp.float32)
            for u in range(4):
                tile = half * 4 + u
                moved = turned(gathered[:, tile * LANES : (tile + 1) * LANES], 8 * u)
                packed = jnp.where(small % BS // 8 == u, moved, packed)
            piece_ref[2 + piece, :, half * LANES : (half + 1) * LANES] = packed
    for piece, (number, lanes) in enumerate([(16, first), (18, first), (17, last), (15, last)]):
        piece_ref[4 + piece, :, 0:LANES] = load(number, lanes)


def stream_into(still_ref, shifted_ref, message_ref, out_ref):
    depth = still_ref.shape[1]
    count = still_ref.shape[2]
    small = lane_of((depth, LANES))
    wide = lane_of((depth, count)) % BS
    columns = []
    for piece in range(2):
        tiles = []
        for half in range(2):
            packed = message_ref[2 + piece, :, half * LANES : (half + 1) * LANES]
            tiles += [turned(packed, -8 * u) for u in range(4)]
        columns.append(jnp.concatenate(tiles, axis=1))
    corners = {15: (4, 0, 127), 17: (5, 31, 96), 18: (6, 96, 31), 16: (7, 127, 0)}
    for number, (shift_x, shift_y, shift_z) in enumerate(velocity_list):
        if number in still:
            value = still_ref[still.index(number)]
        else:
            value = shifted_ref[x_order.index(number)]
        value = turned(value, shift_y * BS + shift_z)
        if shift_z != 0:
            chosen, piece, edge = (z_upward, 0, 0) if shift_z == 1 else (z_downward, 1, BS - 1)
            column = turned(columns[piece], edge - chosen.index(number) + BS * shift_y)
            value = jnp.where(wide == edge, column, value)
        out_ref[number] = value
        if shift_y != 0:
            chosen, piece, lanes, edge = (
                (y_upward, 0, slice(0, LANES), 0)
                if shift_y == 1
                else (y_downward, 1, slice(count - LANES, count), LANES - BS)
            )
            j = chosen.index(number)
            begin = j // 4 * LANES
            row = message_ref[piece, :, begin : begin + LANES]
            row = turned(row, edge - j % 4 * BS + shift_z)
            keep = small // BS == edge // BS
            if shift_z != 0:
                keep = keep & (small % BS != (0 if shift_z == 1 else BS - 1))
            old = value[:, lanes]
            fixed = jnp.where(keep, row, old)
            if number in corners:
                slot, lane_to, lane_from = corners[number]
                corner = turned(message_ref[slot, :, 0:LANES], lane_to - lane_from)
                fixed = jnp.where(small == lane_to, corner, fixed)
            out_ref[number, :, lanes] = fixed


def window_kernel(
    blocks, ring, target_ref, start_ref, field_ref, density_ref,
    still_ref, moving_ref, shifted_ref, up_ref, down_ref, low_ref, high_ref,
    piece_ref, send_ref, got_ref, edge_send, edge_got, send_sem, got_sem,
):
    mesh_ids = pl.DeviceIdType.MESH
    me = lax.axis_index("blk")
    side = lax.axis_index("obs")
    right = lax.rem(side + 1, ring)
    left = lax.rem(side + ring - 1, ring)
    barrier = pltpu.get_barrier_semaphore()

    def greet(distance, carry):
        peer = lax.rem(me + distance, blocks)
        pl.semaphore_signal(barrier, inc=1, device_id=(peer, side), device_id_type=mesh_ids)
        return carry

    for beside in (left, right):
        pl.semaphore_signal(barrier, inc=1, device_id=(me, beside), device_id_type=mesh_ids)
    lax.fori_loop(1, blocks, greet, 0)
    field_ref[...] = start_ref[...]
    pl.semaphore_wait(barrier, blocks + 1)

    def one_step(step, carry):
        collide_all(field_ref, still_ref, moving_ref, up_ref, down_ref)
        edges = [
            pltpu.make_async_remote_copy(
                src_ref=source,
                dst_ref=into.at[step],
                send_sem=edge_send.at[step, way],
                recv_sem=edge_got.at[step, way],
                device_id=(me, beside),
                device_id_type=mesh_ids,
            )
            for way, (source, into, beside) in enumerate(
                [(up_ref, low_ref, right), (down_ref, high_ref, left)]
            )
        ]
        for edge in edges:
            edge.start()
        for edge in edges:
            edge.wait()
        pack_pieces(
            still_ref, moving_ref, low_ref.at[step], high_ref.at[step], shifted_ref, piece_ref
        )

        def copy_to(distance):
            return pltpu.make_async_remote_copy(
                src_ref=send_ref.at[distance],
                dst_ref=got_ref.at[step, me],
                send_sem=send_sem.at[step, distance],
                recv_sem=got_sem.at[step, distance],
                device_id=(lax.rem(me + distance, blocks), side),
                device_id_type=mesh_ids,
            )

        def fill(distance, inner):
            peer = lax.rem(me + distance, blocks)
            near = jnp.zeros((send_ref.shape[1], LANES), jnp.float32)
            rest = near
            for piece in range(8):
                wanted = target_ref[piece] == peer
                near = jnp.where(wanted, piece_ref[piece, :, 0:LANES], near)
                if piece < 4:
                    rest = jnp.where(wanted, piece_ref[piece, :, LANES:FACE], rest)
            send_ref[distance, :, 0:LANES] = near
            send_ref[distance, :, LANES:FACE] = rest
            return inner

        def begin(distance, inner):
            copy_to(distance).start()
            return inner

        def finish(distance, inner):
            copy_to(distance).wait()
            return inner

        lax.fori_loop(1, blocks, fill, 0)
        lax.fori_loop(1, blocks, begin, 0)
        lax.fori_loop(1, blocks, finish, 0)

        def choose(distance, held):
            peer = lax.rem(me + distance, blocks)
            near = got_ref[step, peer, :, 0:LANES]
            rest = got_ref[step, peer, :, LANES:FACE]
            wanted = [target_ref[piece] == peer for piece in range(8)]
            return tuple(
                jnp.where(wanted[at % 8], near if at < 8 else rest, held[at]) for at in range(12)
            )

        blank = jnp.zeros((send_ref.shape[1], LANES), jnp.float32)
        held = lax.fori_loop(1, blocks, choose, (blank,) * 12)
        for at in range(12):
            half = at // 8 * LANES
            piece_ref[at % 8, :, half : half + LANES] = held[at]
        stream_into(still_ref, shifted_ref, piece_ref, field_ref)
        total = field_ref[0]
        for number in range(1, 19):
            total = total + field_ref[number]
        density_ref[step] = total
        return carry

    lax.fori_loop(0, STEPS, one_step, 0)


def call(kernel, outs, scalars, *arrays, scratch=()):
    vmem = pl.BlockSpec(memory_space=pltpu.VMEM)
    smem = pl.BlockSpec(memory_space=pltpu.SMEM)
    shapes = [jax.ShapeDtypeStruct(shape, jnp.float32) for shape in outs]
    return pl.pallas_call(
        kernel,
        out_shape=shapes,
        in_specs=[smem] * len(scalars) + [vmem] * len(arrays),
        out_specs=[vmem] * len(outs),
        scratch_shapes=[pltpu.VMEM(shape, jnp.float32) for shape in scratch],
    )(*scalars, *arrays)


def transform_table():
    moments = jnp.arange(SAMPLES, dtype=jnp.int32)[:, None]
    harmonics = jnp.arange(BINS, dtype=jnp.int32)[None, :] + 1
    turns = moments * harmonics % SAMPLES
    phases = turns.astype(jnp.float32) * (2.0 * math.pi / SAMPLES)
    return jnp.concatenate([jnp.cos(phases), -jnp.sin(phases)], axis=1).astype(jnp.bfloat16)


def greet_peers(blocks):
    me = lax.axis_index("blk")
    side = lax.axis_index("obs")
    barrier = pltpu.get_barrier_semaphore()

    def greet(distance, carry):
        pl.semaphore_signal(
            barrier, inc=1, device_id=(lax.rem(me + distance, blocks), side),
            device_id_type=pl.DeviceIdType.MESH,
        )
        return carry

    lax.fori_loop(1, blocks, greet, 0)
    return barrier


def swap_pieces(blocks, send_ref, got_ref, send_sem, got_sem):
    me = lax.axis_index("blk")
    side = lax.axis_index("obs")

    def copy_to(distance):
        peer = lax.rem(me + distance, blocks)
        return pltpu.make_async_remote_copy(
            src_ref=send_ref.at[peer],
            dst_ref=got_ref.at[me],
            send_sem=send_sem.at[distance],
            recv_sem=got_sem.at[distance],
            device_id=(peer, side),
            device_id_type=pl.DeviceIdType.MESH,
        )

    def begin(distance, inner):
        copy_to(distance).start()
        return inner

    def finish(distance, inner):
        copy_to(distance).wait()
        return inner

    lax.fori_loop(1, blocks, begin, 0)
    lax.fori_loop(1, blocks, finish, 0)


def exchange_kernel(blocks, source_ref, out_ref, got_ref, send_sem, got_sem):
    me = lax.axis_index("blk")
    barrier = greet_peers(blocks)
    got_ref[me] = source_ref[me]
    pl.semaphore_wait(barrier, blocks - 1)
    swap_pieces(blocks, source_ref, got_ref, send_sem, got_sem)
    out_ref[...] = got_ref[...]


def radiate_kernel(
    blocks, panel_ref, listen_ref, out_ref,
    real_ref, imag_ref, full_ref, send_ref, got_ref, send_sem, got_sem,
):
    barrier = greet_peers(blocks)
    listeners = listen_ref.shape[1]
    real_ref[...] = jnp.zeros_like(real_ref)
    imag_ref[...] = jnp.zeros_like(imag_ref)
    step_angle = 2.0 * math.pi / SAMPLES / sound_speed

    def accumulate(block_number, carry):
        begin = pl.multiple_of(block_number * 8, 8)
        panel = panel_ref[pl.ds(begin, 8), :]
        distance_sq = None
        facing = None
        for axis in range(3):
            at = 4 * BINS + axis
            offset = listen_ref[axis : axis + 1, :] - panel[:, at : at + 1]
            square = offset * offset
            along = panel[:, at + 3 : at + 4] * offset
            distance_sq = square if distance_sq is None else distance_sq + square
            facing = along if facing is None else facing + along
        distance = jnp.sqrt(distance_sq)
        far_term = facing / (4.0 * math.pi * sound_speed * distance_sq)
        ratio = sound_speed / distance
        angle = step_angle * distance
        turn_cos = jnp.cos(angle)
        turn_sin = jnp.sin(angle)
        wave_cos = far_term * turn_cos
        wave_sin = far_term * turn_sin
        for k in range(BINS):
            press_real = panel[:, k : k + 1]
            press_imag = panel[:, BINS + k : BINS + k + 1]
            rate_real = panel[:, 2 * BINS + k : 2 * BINS + k + 1]
            rate_imag = panel[:, 3 * BINS + k : 3 * BINS + k + 1]
            mixed_real = rate_real + ratio * press_real
            mixed_imag = rate_imag + ratio * press_imag
            real_ref[k] += mixed_real * wave_cos + mixed_imag * wave_sin
            imag_ref[k] += mixed_imag * wave_cos - mixed_real * wave_sin
            if k + 1 < BINS:
                wave_cos, wave_sin = (
                    wave_cos * turn_cos - wave_sin * turn_sin,
                    wave_sin * turn_cos + wave_cos * turn_sin,
                )
        return carry

    lax.fori_loop(0, panel_ref.shape[0] // 8, accumulate, 0)
    both = jnp.concatenate([jnp.sum(real_ref[...], axis=1), jnp.sum(imag_ref[...], axis=1)], axis=0)
    full_ref[...] = both.T
    chunk = out_ref.shape[0]
    for number in range(blocks):
        send_ref[number] = full_ref[number * chunk : (number + 1) * chunk]
    me = lax.axis_index("blk")
    got_ref[me] = send_ref[me]
    pl.semaphore_wait(barrier, blocks - 1)
    swap_pieces(blocks, send_ref, got_ref, send_sem, got_sem)
    out_ref[...] = jnp.sum(got_ref[...], axis=0)


def route_slots(payload, owners, alive_slot, blocks):
    count_slots = payload.shape[0]
    capacity = -(-count_slots // blocks)
    target = owners // P_OWN
    member = (
        (target[:, None] == jnp.arange(blocks, dtype=jnp.int32)[None, :]) & alive_slot[:, None]
    ).astype(jnp.int32)
    before = jnp.cumsum(member, axis=0) - member
    order_within = jnp.sum(before * member, axis=1)
    slot_label = jnp.where(alive_slot, target * capacity + order_within, -1)
    matches = slot_label[:, None] == jnp.arange(blocks * capacity, dtype=jnp.int32)[None, :]
    source = jnp.sum(
        jnp.where(matches, jnp.arange(count_slots, dtype=jnp.int32)[:, None], 0), axis=0
    )
    filled = jnp.any(matches, axis=0)
    outgoing = jnp.take(payload, source, axis=0).reshape(blocks, capacity, payload.shape[1])
    spots = jnp.where(filled, jnp.take(owners, source) % P_OWN, -1).reshape(blocks, capacity, 1)
    return jnp.concatenate([outgoing, spots.astype(jnp.bfloat16)], axis=2)


def settle(incoming):
    width = incoming.shape[-1] - 1
    flat = incoming.reshape(-1, width + 1)
    spots = flat[:, width].astype(jnp.int32)
    choose = (spots[:, None] == jnp.arange(P_OWN, dtype=jnp.int32)[None, :]).astype(jnp.bfloat16)
    return jnp.einsum(
        "rp,rw->pw", choose, flat[:, :width], preferred_element_type=jnp.float32
    ).astype(jnp.bfloat16)


def body(
    populations,
    block_faces,
    block_edges,
    probe_cell,
    history,
    panel_count,
    panel_owner,
    panel_pos,
    panel_normal,
    observers,
):
    blocks = lax.axis_size("blk")
    lattice_state = populations[0]
    slab_depth = lattice_state.shape[1]
    lane_count = lattice_state.shape[2]
    targets = jnp.concatenate([block_faces[0], block_edges[0]])
    ring = lax.axis_size("obs")
    still_shape = (len(still), slab_depth, lane_count)
    moving_shape = (len(x_order), slab_depth, lane_count)
    edge_shape = (5, 1, lane_count)
    vmem = pl.BlockSpec(memory_space=pltpu.VMEM)
    scratch = [
        still_shape, moving_shape, moving_shape, edge_shape, edge_shape,
        (STEPS,) + edge_shape, (STEPS,) + edge_shape,
        (8, slab_depth, FACE), (blocks, slab_depth, FACE), (STEPS, blocks, slab_depth, FACE),
    ]
    lattice_state, densities = pl.pallas_call(
        functools.partial(window_kernel, blocks, ring),
        out_shape=[
            jax.ShapeDtypeStruct((19, slab_depth, lane_count), jnp.float32),
            jax.ShapeDtypeStruct((STEPS, slab_depth, lane_count), jnp.float32),
        ],
        in_specs=[pl.BlockSpec(memory_space=pltpu.SMEM), vmem],
        out_specs=[vmem, vmem],
        scratch_shapes=[pltpu.VMEM(shape, jnp.float32) for shape in scratch]
        + [pltpu.SemaphoreType.DMA((STEPS, 2))] * 2
        + [pltpu.SemaphoreType.DMA((STEPS, blocks))] * 2,
        compiler_params=pltpu.CompilerParams(collective_id=0, has_side_effects=True),
    )(targets, lattice_state)
    populations_out = lattice_state.reshape(1, 19, slab_depth, lane_count)
    readings = [jnp.take(density.reshape(-1), probe_cell) for density in densities]
    gained = pressure_gain * (jnp.stack(readings, axis=1) - 1.0)
    previous = jnp.concatenate(
        [history[:, SAMPLES - 1 : SAMPLES].astype(jnp.float32), gained[:, :-1]], axis=1
    )
    rate_values = gained - previous
    recent = jnp.concatenate(
        [
            history[:, STEPS:SAMPLES],
            gained.astype(jnp.bfloat16),
            history[:, SAMPLES + STEPS :],
            rate_values.astype(jnp.bfloat16),
        ],
        axis=1,
    )
    transform = transform_table()
    count_slots = recent.shape[0]
    alive_slot = jnp.arange(count_slots, dtype=jnp.int32) < panel_count[0]
    outgoing = route_slots(recent, panel_owner, alive_slot, blocks)
    incoming = pl.pallas_call(
        functools.partial(exchange_kernel, blocks),
        out_shape=jax.ShapeDtypeStruct(outgoing.shape, outgoing.dtype),
        in_specs=[vmem],
        out_specs=vmem,
        scratch_shapes=[pltpu.VMEM(outgoing.shape, outgoing.dtype)]
        + [pltpu.SemaphoreType.DMA((blocks,))] * 2,
        compiler_params=pltpu.CompilerParams(collective_id=1, has_side_effects=True),
    )(outgoing)
    owned = settle(incoming).reshape(P_OWN, 2, SAMPLES)
    spectra = (
        jnp.einsum("pgt,tk->pgk", owned, transform, preferred_element_type=jnp.float32)
        .astype(jnp.bfloat16)
        .reshape(P_OWN, 4 * BINS)
    )
    panels = jnp.concatenate([spectra, panel_pos.T, panel_normal.T], axis=1)
    gathered = lax.all_gather(panels, "obs", axis=0, tiled=True).astype(jnp.float32)
    listeners = observers.shape[1]
    chunk = listeners // blocks
    spectrum = pl.pallas_call(
        functools.partial(radiate_kernel, blocks),
        out_shape=jax.ShapeDtypeStruct((chunk, 2 * BINS), jnp.float32),
        in_specs=[vmem, vmem],
        out_specs=vmem,
        scratch_shapes=[
            pltpu.VMEM(shape, jnp.float32)
            for shape in [
                (BINS, 8, listeners), (BINS, 8, listeners), (listeners, 2 * BINS),
                (blocks, chunk, 2 * BINS), (blocks, chunk, 2 * BINS),
            ]
        ]
        + [pltpu.SemaphoreType.DMA((blocks,))] * 2,
        compiler_params=pltpu.CompilerParams(collective_id=2, has_side_effects=True),
    )(gathered, observers)
    return (populations_out, spectrum[None])


def solution(mesh):
    placed = (
        P("blk", None, "obs", None),
        P("blk", None),
        P("blk", None),
        P(("blk", "obs")),
        P(("blk", "obs"), None),
        P(("blk", "obs")),
        P(("blk", "obs")),
        P(None, ("blk", "obs")),
        P(None, ("blk", "obs")),
        P(None, "obs"),
    )
    return jax.shard_map(
        body,
        mesh=mesh,
        in_specs=placed,
        out_specs=(P("blk", None, "obs", None), P("obs", "blk", None)),
        check_vma=False,
    )
```
